512 devices in a mesh: rows: 128 (over y_lo, x, z), cols: 4 (over y_hi, core).
Axes of the slice: x: 4, y: 4 (y_hi: 2, y_lo: 2; y = y_hi * 2 + y_lo), z: 16, core: 2. Of those that a mesh axis runs over, the one named last changes fastest.
Arguments:
- grad_out: bfloat16 [512, 512, 192], P(('rows', 'cols')), may hold values from -6 to 6
- inputs: bfloat16 [1024, 1024, 192], P('rows', 'cols'), may hold values from -6 to 6
- weight: bfloat16 [3, 3, 192, 192], replicated, may hold values from -0.15625 to 0.15625
Outputs:
- input_grad: bfloat16 [1024, 1024, 192], P('rows', 'cols')
- filter_grad: float32 [3, 3, 192, 192], replicated
The draws below stay inside these ranges and needn't reach their ends.
All inputs are finite; a program needn't handle non-finite values.
Results may differ from the reference program's by a relative error of at most 0.0028.
Values may be sent and summed in bfloat16 or wider, within the bound.
A program may use at most 64 MiB of HBM per device.

```python
import jax
import jax.numpy as jnp
from jax import lax

C = 192
ROWS_DEV = 8
HEIGHT = 1024
WIDTH = 1024
POSITIONS = 262144


def steps_of(key, dims, cuts, least, largest):
    def one(dim, parts):
        draws = jax.random.uniform(jax.random.fold_in(jax.random.fold_in(key, 6), dim), (parts,), jnp.float32, least / len(cuts), largest / len(cuts))
        return jnp.repeat(jnp.exp(draws), dims[dim] // parts).reshape((-1,) + (1,) * (len(dims) - dim - 1))

    level = one(*cuts[0])
    for cut in cuts[1:]:
        level = level * one(*cut)
    return level


def bell_draw(rng, extent, scale, most, shards=(), kind=jnp.bfloat16):
    drawn = jax.random.normal(rng, extent, jnp.float32) * scale
    if len(shards) > 0:
        drawn = steps_of(rng, extent, shards, -0.22, 0.18) * drawn
    return jnp.clip(drawn, min=-most, max=most).astype(kind)


def setup_inputs(seed: int = 0) -> dict:
    key_of = jax.random.split(jax.random.key(seed), 4)
    return {
        "grad_out": bell_draw(key_of[0], (HEIGHT // 2, WIDTH // 2, C), 1.0, 6.0, ((0, 512),)),
        "inputs": bell_draw(key_of[1], (HEIGHT, WIDTH, C), 1.0, 6.0, ((0, 128), (1, 4))),
        "weight": bell_draw(key_of[2], (3, 3, C, C), (9 * C) ** -0.5, 0.15625),
    }


def tap_products(out_block, flat_weight):
    chans = flat_weight.shape[0]
    flat = out_block.reshape(-1, chans)
    products = jnp.dot(flat, flat_weight, preferred_element_type=jnp.float32)
    return products.reshape(out_block.shape[0], out_block.shape[1], 3, 3, chans)

def assemble(products, count_rows, count_cols):
    rows_even = products[:count_rows, :, 1]
    rows_odd = products[:count_rows, :, 2] + products[1:count_rows + 1, :, 0]

    def columns(mixed):
        even = mixed[:, :count_cols, 1]
        odd = mixed[:, :count_cols, 2] + mixed[:, 1:count_cols + 1, 0]
        return jnp.stack([even, odd], axis=2)
    placed = jnp.stack([columns(rows_even), columns(rows_odd)], axis=1)
    return placed.reshape(2 * count_rows, 2 * count_cols, products.shape[-1])

def filter_terms(input_band, out_band, row_taps):
    count_rows, count_cols, chans = out_band.shape
    split = input_band.reshape(count_rows + 1, 2, count_cols + 1, 2, chans)
    offsets = ((0, 0), (0, 1), (1, 0))
    pieces = []
    for row_tap in row_taps:
        start_row, parity_row = offsets[row_tap]
        for col_tap in range(3):
            start_col, parity_col = offsets[col_tap]
            pieces.append(split[start_row:start_row + count_rows, parity_row, start_col:start_col + count_cols, parity_col])
    stacked = jnp.stack(pieces, axis=2).reshape(count_rows * count_cols, len(pieces) * chans)
    flat_out = out_band.reshape(count_rows * count_cols, chans)
    return lax.dot_general(stacked, flat_out, (((0,), (0,)), ((), ())), preferred_element_type=jnp.float32)

def reference(grad_out, inputs, weight):
    half_rows, half_cols, chans = grad_out.shape
    band_rows = ROWS_DEV // 2
    flat_weight = jnp.transpose(weight, (3, 0, 1, 2)).reshape(chans, 9 * chans)
    padded_out = jnp.pad(grad_out, ((0, 1), (0, 1), (0, 0)))
    padded_in = jnp.pad(inputs, ((1, 1), (1, 1), (0, 0)))

    def step(total, index):
        start = (index * band_rows).astype(jnp.int32)
        out_block = lax.dynamic_slice_in_dim(padded_out, start, band_rows + 1, 0)
        input_band = lax.dynamic_slice_in_dim(padded_in, (2 * start).astype(jnp.int32), 2 * band_rows + 2, 0)
        block = assemble(tap_products(out_block, flat_weight), band_rows, half_cols).astype(jnp.bfloat16)
        terms = filter_terms(input_band, out_block[:band_rows, :half_cols], (0, 1, 2))
        return (total + terms, block)
    total, blocks = lax.scan(step, jnp.zeros((9 * chans, chans), jnp.float32), jnp.arange(half_rows // band_rows, dtype=jnp.int32))
    input_grad = blocks.reshape(2 * half_rows, 2 * half_cols, chans)
    filter_grad = total.reshape(3, 3, chans, chans) / jnp.sqrt(jnp.float32(POSITIONS))
    return (input_grad, filter_grad)
```

```python
import functools

import jax
import jax.numpy as jnp
from jax import lax
from jax.experimental import pallas as pl
from jax.experimental.pallas import tpu as pltpu
from jax.sharding import Mesh
from jax.sharding import PartitionSpec as P

MESH = pl.DeviceIdType.MESH
YLO, X, Z, YHI, CORE = "rows_0", "rows_1", "rows_2", "cols_0", "cols_1"
COLS = (YHI, CORE)
ROWS = (YLO, X, Z)
F32, BF16 = jnp.float32, jnp.bfloat16
C = 192
TAP_ROWS = C + C // 2
HALF = 9 * TAP_ROWS // 2


def dot_nn(a, b):
    return lax.dot_general(a, b, (((1,), (0,)), ((), ())), preferred_element_type=F32)


def dot_nt(a, b):
    return lax.dot_general(a, b, (((1,), (1,)), ((), ())), preferred_element_type=F32)


def iota(shape, dim):
    return lax.broadcasted_iota(jnp.int32, shape, dim)


def kernel(sizes, g_hbm, x_hbm, w_hbm, ig_hbm, fg_hbm, gsend, gcat, gshift, xin, w, xd, ig2, igo, terms, dbuf,
           sbuf, rbuf, acc, zbuf, zfar, zown, fin, agbuf, fgo,
           load_sem, gs_sem, gr_sem, ds_sem, dr_sem, xs_sem, xr_sem, ns_sem, nr_sem, fs_sem, fr_sem,
           as_sem, ar_sem, os_sem, or_sem, ps_sem, pr_sem, out_sem):
    nyl, nx, nz, nyh, nzl, chunk, scale = sizes
    planes = nx * nyl * nyh
    nzh = nz // nzl
    piece = chunk // nzl
    ny = nyl * nyh
    rows = nyl * nx * nz
    yl, x, z, yh, core = (lax.axis_index(a) for a in (YLO, X, Z, YHI, CORE))
    row = (yl * nx + x) * nz + z
    col = yh * 2 + core
    y = yh * nyl + yl
    me = x * ny + y
    zh, zl = z // nzl, z % nzl

    load_g = pltpu.make_async_copy(g_hbm, gsend.at[0:C], load_sem.at[0])
    load_x = pltpu.make_async_copy(x_hbm, xin, load_sem.at[1])
    load_w = pltpu.make_async_copy(w_hbm, w, load_sem.at[2])
    load_g.start()
    load_x.start()
    load_w.start()

    def at_row(r):
        return {YLO: r // (nx * nz), X: (r // nz) % nx, Z: r % nz}

    def at_col(c):
        return {YHI: c // 2, CORE: c % 2}

    def at_plane(dx, dy):
        px, py = (x + dx) % nx, (y + dy) % ny
        return px * ny + py, {X: px, YHI: py // nyl, YLO: py % nyl}

    offsets = [(dx, dy) for dx in range(nx) for dy in range(ny) if (dx, dy) != (0, 0)]
    offsets.sort(key=lambda o: -(min(o[0], nx - o[0]) + min(o[1], ny - o[1])))

    barrier = pltpu.get_barrier_semaphore()

    def greet(where):
        pl.semaphore_signal(barrier, inc=1, device_id=where, device_id_type=MESH)

    for d in range(1, nzh):
        greet({Z: ((zh + d) % nzh) * nzl + zl})
    for d in range(1, nzl):
        greet({Z: zh * nzl + (zl + d) % nzl})
    for dx, dy in offsets:
        greet(at_plane(dx, dy)[1])
    greet({CORE: 1 - core})
    greet({CORE: 1 - core, YHI: 1 - yh})

    @pl.when(row < rows - 1)
    def _():
        greet(at_row(row + 1) | at_col(0))

    met = (nzh - 1) + (nzl - 1) + len(offsets) + 2

    load_g.wait()
    blocks = 4
    width = gsend.shape[1]
    sel_row, sel_col = iota((16, width), 0), iota((16, width), 1)
    for c in range(blocks - 1):
        hit = sel_col == 128 * (c + 1)
        first = jnp.where(hit & (sel_row == 0), 1.0, 0.0).astype(BF16)
        second = jnp.where(hit & (sel_row == 1), 1.0, 0.0).astype(BF16)
        tile = dot_nt(first, gsend[0:128, :]) + dot_nt(second, gsend[64:192, :])
        gsend[C : C + 16, 128 * c : 128 * c + 128] = tile.astype(BF16)
    gsend[C : C + 16, 128 * (blocks - 1) :] = jnp.zeros((16, 128), BF16)
    own = pl.multiple_of(col * 128, 128)
    gcat[:, pl.ds(own, 128)] = gsend[:, pl.ds(own, 128)]

    @pl.when(row == rows - 1)
    def _():
        gcat[:, 512:640] = jnp.zeros((C + 16, 128), BF16)

    load_x.wait()
    r256, c256 = iota((256, 256), 0), iota((256, 256), 1)
    part = jnp.where(r256 == 2 * (c256 % 128) + c256 // 128, 1.0, 0.0).astype(BF16)
    join = jnp.where(c256 == 2 * (r256 % 128) + r256 // 128, 1.0, 0.0).astype(BF16)
    for p in range(8):
        both = dot_nn(xin[p], part).astype(BF16)
        lanes = slice(128 * (p // 2), 128 * (p // 2) + 128)
        xd[p % 2, 0, :, lanes] = both[:, 0:128]
        xd[p % 2, 1, :, lanes] = both[:, 128:256]

    @pl.when((col == 0) & (row > 0))
    def _():
        pl.semaphore_wait(barrier, met + 4)

    @pl.when((col != 0) | (row == 0))
    def _():
        pl.semaphore_wait(barrier, met)

    def g_copy(c, slot, where, sem):
        return pltpu.make_async_remote_copy(
            src_ref=gsend.at[:, pl.ds(pl.multiple_of(c * 128, 128), 128)],
            dst_ref=gcat.at[:, pl.ds(pl.multiple_of(slot * 128, 128), 128)],
            send_sem=gs_sem.at[sem], recv_sem=gr_sem.at[slot], device_id=where, device_id_type=MESH)

    peers = [(col + d) % 4 for d in (2, 3, 1)]
    g_sent = [g_copy(c, col, at_col(c), n) for n, c in enumerate(peers)]
    for copy in g_sent:
        copy.start()
    upward = [g_copy(c, 4, at_row(row - 1) | at_col(c), 3 + c) for c in range(4)]

    @pl.when((col == 0) & (row > 0))
    def _():
        for copy in upward:
            copy.start()

    for d in (1, 2, 3):
        g_copy(0, (col + d) % 4, at_col(0), 0).wait_recv()

    @pl.when(row < rows - 1)
    def _():
        g_copy(0, 4, at_col(0), 0).wait_recv()

    r128, c128 = iota((128, 128), 0), iota((128, 128), 1)
    shift = jnp.where(r128 == c128 + 1, 1.0, 0.0).astype(BF16)
    eye = jnp.where(r128 == c128, 1.0, 0.0).astype(BF16)
    for i in range(5):
        lanes = slice(128 * i, 128 * i + 128)
        moved = dot_nn(gcat[0:C, lanes], shift)
        tile = gcat[C : C + 16, lanes].astype(F32)
        edge0 = jnp.where(r128 == 127, tile[0:1, :], 0.0).astype(BF16)
        edge1 = jnp.where(r128 == 127, tile[1:2, :], 0.0).astype(BF16)
        gshift[0:128, lanes] = (moved[0:128] + dot_nt(eye, edge0)).astype(BF16)
        gshift[128:192, lanes] = (moved[128:192] + dot_nt(eye, edge1)[64:128]).astype(BF16)

    def grad(down, right):
        ref = gshift if right else gcat
        return ref, slice(128 * down, 128 * down + 512)

    taps = {0: (1, 1), 1: (0, 0), 2: (1, 0)}
    low = iota((C // 2, 128), 1) < 64
    for t in range(9):
        (row_par, down), (col_par, right) = taps[t // 3], taps[t % 3]
        ref, lanes = grad(down, right)
        lhs = xd[row_par, col_par]
        main = dot_nt(lhs, ref[0:128, lanes])
        rest = dot_nt(lhs, ref[64:192, lanes])
        rest = jnp.where(low, pltpu.roll(rest[0 : C // 2], 64, 1), rest[C // 2 : C])
        start = TAP_ROWS * t
        for begin, values in ((start, main), (start + C, rest)):
            count = values.shape[0]
            cut = min(max(HALF - begin, 0), count)
            if cut > 0:
                terms[0, begin : begin + cut] = values[0:cut]
            if cut < count:
                terms[1, begin + cut - HALF : begin + count - HALF] = values[cut:]
    spare = planes * chunk - HALF
    if spare:
        for h in range(2):
            terms[h, HALF:] = jnp.zeros((spare, 128), F32)

    pair = pltpu.make_async_remote_copy(
        src_ref=terms.at[1 - core], dst_ref=dbuf, send_sem=ds_sem, recv_sem=dr_sem,
        device_id={CORE: 1 - core}, device_id_type=MESH)
    pair.start()
    pair.wait_recv()

    def plane_copy(n, source, slot, where):
        return pltpu.make_async_remote_copy(
            src_ref=sbuf.at[source], dst_ref=rbuf.at[slot], send_sem=xs_sem.at[n], recv_sem=xr_sem.at[slot],
            device_id=where, device_id_type=MESH)

    plane_sent = []
    for n, (dx, dy) in enumerate(offsets):
        q, where = at_plane(dx, dy)
        at = pl.ds(pl.multiple_of(q * chunk, chunk), chunk)
        sbuf[q] = (terms[core, at, :] + dbuf[at, :]).astype(BF16)
        copy = plane_copy(n, q, me, where)
        copy.start()
        plane_sent.append(copy)
    at = pl.ds(pl.multiple_of(me * chunk, chunk), chunk)
    acc[...] = terms[core, at, :] + dbuf[at, :]

    load_w.wait()

    def tap(a, b):
        return w[3 * a + b]

    def apply(pairs):
        total = None
        for (a, b), (down, right) in pairs:
            ref, lanes = grad(down, right)
            one = dot_nn(tap(a, b), ref[0:C, lanes])
            total = one if total is None else total + one
        return total.astype(BF16)

    plan = {
        (0, 0): [((1, 1), (0, 0))],
        (0, 1): [((1, 2), (0, 0)), ((1, 0), (0, 1))],
        (1, 0): [((2, 1), (0, 0)), ((0, 1), (1, 0))],
        (1, 1): [((2, 2), (0, 0)), ((2, 0), (0, 1)), ((0, 2), (1, 0)), ((0, 0), (1, 1))],
    }
    for (row_par, col_par), pairs in plan.items():
        placed = apply(pairs)
        for i in range(4):
            ig2[row_par, i, :, 128 * col_par : 128 * col_par + 128] = placed[:, 128 * i : 128 * i + 128]
    for p in range(8):
        igo[p] = dot_nn(ig2[p % 2, p // 2], join).astype(BF16)
    store_ig = pltpu.make_async_copy(igo, ig_hbm, out_sem.at[0])
    store_ig.start()

    total = acc[...]
    for dx, dy in reversed(offsets):
        q, where = at_plane(dx, dy)
        plane_copy(0, q, q, where).wait_recv()
        total += rbuf[q].astype(F32)
    acc[...] = total

    def near_copy(n, k, slot, where):
        return pltpu.make_async_remote_copy(
            src_ref=acc.at[pl.ds(pl.multiple_of(k * piece, 8), piece)], dst_ref=zbuf.at[slot],
            send_sem=ns_sem.at[n], recv_sem=nr_sem.at[slot], device_id={Z: where}, device_id_type=MESH)

    near_sent = []
    for d in range(1, nzl):
        k = (zl + d) % nzl
        copy = near_copy(d - 1, k, zl, zh * nzl + k)
        copy.start()
        near_sent.append(copy)
    total = acc[pl.ds(pl.multiple_of(zl * piece, 8), piece)]
    for d in range(1, nzl):
        k = (zl + d) % nzl
        near_copy(0, k, k, z).wait_recv()
        total += zbuf[k]
    zown[...] = total
    zfar[zh] = total

    def far_copy(n, slot, where):
        return pltpu.make_async_remote_copy(
            src_ref=zown, dst_ref=zfar.at[slot], send_sem=fs_sem.at[n], recv_sem=fr_sem.at[slot],
            device_id={Z: where}, device_id_type=MESH)

    far_sent = []
    for n, d in enumerate(sorted(range(1, nzh), key=lambda d: -min(d, nzh - d))):
        copy = far_copy(n, zh, ((zh + d) % nzh) * nzl + zl)
        copy.start()
        far_sent.append(copy)
    for d in range(1, nzh):
        far_copy(0, (zh + d) % nzh, z).wait_recv()
    total = zfar[0]
    for k in range(1, nzh):
        total += zfar[k]
    mine = pl.ds(pl.multiple_of(zl * piece, 8), piece)
    fin[mine] = total

    def gather_copy(n, k, where):
        part_of = pl.ds(pl.multiple_of(k * piece, 8), piece)
        return pltpu.make_async_remote_copy(
            src_ref=fin.at[part_of], dst_ref=fin.at[part_of], send_sem=as_sem.at[n], recv_sem=ar_sem.at[k],
            device_id={Z: where}, device_id_type=MESH)

    gather_sent = []
    for d in range(1, nzl):
        copy = gather_copy(d - 1, zl, zh * nzl + (zl + d) % nzl)
        copy.start()
        gather_sent.append(copy)
    for d in range(1, nzl):
        gather_copy(0, (zl + d) % nzl, z).wait_recv()

    def ag_at(h, q):
        return agbuf.at[h, pl.ds(pl.multiple_of(q * chunk, chunk), chunk)]

    def spread_copy(n, q, where):
        return pltpu.make_async_remote_copy(
            src_ref=ag_at(core, q), dst_ref=ag_at(core, q), send_sem=os_sem.at[n], recv_sem=or_sem.at[q],
            device_id=where, device_id_type=MESH)

    def pass_copy(q, half):
        return pltpu.make_async_remote_copy(
            src_ref=ag_at(half, q), dst_ref=ag_at(half, q), send_sem=ps_sem.at[q], recv_sem=pr_sem.at[q],
            device_id={CORE: 1 - core}, device_id_type=MESH)

    agbuf[core, pl.ds(pl.multiple_of(me * chunk, chunk), chunk)] = fin[...].astype(BF16)
    spread_sent = []
    for n, (dx, dy) in enumerate(offsets):
        copy = spread_copy(n, me, at_plane(dx, dy)[1])
        copy.start()
        spread_sent.append(copy)
    pass_sent = [pass_copy(me, core)]
    pass_sent[0].start()
    for dx, dy in reversed(offsets):
        q = at_plane(dx, dy)[0]
        spread_copy(0, q, {}).wait_recv()
        copy = pass_copy(q, core)
        copy.start()
        pass_sent.append(copy)
    for q in range(planes):
        pass_copy(q, 1 - core).wait_recv()

    def packed(begin, count):
        cut = min(max(HALF - begin, 0), count)
        parts = []
        if cut > 0:
            parts.append(agbuf[0, begin : begin + cut])
        if cut < count:
            parts.append(agbuf[1, begin + cut - HALF : begin + count - HALF])
        values = parts[0] if len(parts) == 1 else jnp.concatenate(parts, axis=0)
        return values.astype(F32) * scale

    for t in range(9):
        start = TAP_ROWS * t
        fgo[t, :, 0:128] = packed(start, C)
        rest = packed(start + C, C // 2)
        fgo[t, 0 : C // 2, 128:C] = rest[:, 0:64]
        fgo[t, C // 2 : C, 128:C] = pltpu.roll(rest, 64, 1)[:, 0:64]
    store_fg = pltpu.make_async_copy(fgo, fg_hbm, out_sem.at[1])
    store_fg.start()

    for copy in g_sent + [pair] + plane_sent + near_sent + far_sent + gather_sent + spread_sent + pass_sent:
        copy.wait_send()

    @pl.when((col == 0) & (row > 0))
    def _():
        for copy in upward:
            copy.wait_send()

    store_ig.wait()
    store_fg.wait()


def near_size(nz):
    return 4 if nz % 4 == 0 and nz > 4 else max(nz // 2, 1)


def per_device(scale, grad_out, inputs, weight):
    nyl, nx, nz, nyh = (lax.axis_size(a) for a in (YLO, X, Z, YHI))
    planes = nx * nyl * nyh
    nzl = near_size(nz)
    chunk = -(-HALF // planes)
    chunk = -(-chunk // 96) * 96
    g = jnp.transpose(grad_out, (0, 2, 1)).reshape(C, grad_out.shape[1])
    xt = jnp.transpose(inputs, (0, 2, 1))
    wt = weight.reshape(9, C, C)
    sizes = (nyl, nx, nz, nyh, nzl, chunk, scale)
    dma = pltpu.SemaphoreType.DMA
    hbm = pl.BlockSpec(memory_space=pl.ANY)
    n = planes - 1
    nzh = nz // nzl
    piece = chunk // nzl
    ig, fg = pl.pallas_call(
        functools.partial(kernel, sizes),
        out_shape=(
            jax.ShapeDtypeStruct(xt.shape, BF16),
            jax.ShapeDtypeStruct((9, C, C), F32),
        ),
        in_specs=[hbm] * 3,
        out_specs=(hbm, hbm),
        scratch_shapes=[
            pltpu.VMEM((C + 16, 512), BF16),
            pltpu.VMEM((C + 16, 640), BF16),
            pltpu.VMEM((C, 640), BF16),
            pltpu.VMEM(xt.shape, BF16),
            pltpu.VMEM((9, C, C), BF16),
            pltpu.VMEM((2, 2, C, 512), BF16),
            pltpu.VMEM((2, 4, C, 256), BF16),
            pltpu.VMEM(xt.shape, BF16),
            pltpu.VMEM((2, planes * chunk, 128), F32),
            pltpu.VMEM((planes * chunk, 128), F32),
            pltpu.VMEM((planes, chunk, 128), BF16),
            pltpu.VMEM((planes, chunk, 128), BF16),
            pltpu.VMEM((chunk, 128), F32),
            pltpu.VMEM((nzl, piece, 128), F32),
            pltpu.VMEM((nzh, piece, 128), F32),
            pltpu.VMEM((piece, 128), F32),
            pltpu.VMEM((chunk, 128), F32),
            pltpu.VMEM((2, planes * chunk, 128), BF16),
            pltpu.VMEM((9, C, C), F32),
            dma((3,)), dma((7,)), dma((5,)), dma, dma, dma((n,)), dma((planes,)),
            dma((nzl,)), dma((nzl,)), dma((nzh,)), dma((nzh,)), dma((nzl,)), dma((nzl,)),
            dma((n,)), dma((planes,)), dma((planes,)), dma((planes,)), dma((2,)),
        ],
        compiler_params=pltpu.CompilerParams(
            collective_id=0, has_side_effects=True, vmem_limit_bytes=48 * 1024 * 1024
        ),
    )(g, xt, wt)
    return jnp.transpose(ig, (0, 2, 1)), fg.reshape(3, 3, C, C)


def solution(mesh):
    split = Mesh(mesh.devices.reshape(2, 4, 16, 2, 2), ROWS + COLS)
    positions = (4 * mesh.shape["rows"]) * (128 * mesh.shape["cols"])
    return jax.shard_map(
        functools.partial(per_device, positions ** -0.5),
        mesh=split,
        in_specs=(P(ROWS + COLS, None, None), P(ROWS, COLS, None), P()),
        out_specs=(P(ROWS, COLS, None), P()),
        check_vma=False,
    )
```

```python
import functools

import jax
import jax.numpy as jnp
from jax import lax
from jax.experimental import pallas as pl
from jax.experimental.pallas import tpu as pltpu
from jax.sharding import Mesh
from jax.sharding import PartitionSpec as P

MESH = pl.DeviceIdType.MESH
YLO, X, Z, YHI, CORE = "rows_0", "rows_1", "rows_2", "cols_0", "cols_1"
COLS = (YHI, CORE)
ROWS = (YLO, X, Z)
F32, BF16 = jnp.float32, jnp.bfloat16
C = 192
TAP_ROWS = C + C // 2
HALF = 9 * TAP_ROWS // 2


def dot_nn(a, b):
    return lax.dot_general(a, b, (((1,), (0,)), ((), ())), preferred_element_type=F32)


def dot_nt(a, b):
    return lax.dot_general(a, b, (((1,), (1,)), ((), ())), preferred_element_type=F32)


def iota(shape, dim):
    return lax.broadcasted_iota(jnp.int32, shape, dim)


def kernel(sizes, g_hbm, x_hbm, w_hbm, igo, agbuf, gsend, gcat, gshift, xin, w, xd, ig2, terms, dbuf,
           sbuf, rbuf, acc, zbuf, zfar, zown, fin,
           load_sem, gs_sem, gr_sem, ds_sem, dr_sem, xs_sem, xr_sem, ns_sem, nr_sem, fs_sem, fr_sem,
           as_sem, ar_sem, os_sem, or_sem, ps_sem, pr_sem):
    nyl, nx, nz, nyh, nzl, chunk = sizes
    planes = nx * nyl * nyh
    nzh = nz // nzl
    piece = chunk // nzl
    ny = nyl * nyh
    rows = nyl * nx * nz
    yl, x, z, yh, core = (lax.axis_index(a) for a in (YLO, X, Z, YHI, CORE))
    row = (yl * nx + x) * nz + z
    col = yh * 2 + core
    y = yh * nyl + yl
    me = x * ny + y
    zh, zl = z // nzl, z % nzl

    load_g = pltpu.make_async_copy(g_hbm, gsend.at[0:C], load_sem.at[0])
    load_x = pltpu.make_async_copy(x_hbm, xin, load_sem.at[1])
    load_w = pltpu.make_async_copy(w_hbm, w, load_sem.at[2])
    load_g.start()
    load_x.start()
    load_w.start()

    def at_row(r):
        return {YLO: r // (nx * nz), X: (r // nz) % nx, Z: r % nz}

    def at_col(c):
        return {YHI: c // 2, CORE: c % 2}

    def at_plane(dx, dy):
        px, py = (x + dx) % nx, (y + dy) % ny
        return px * ny + py, {X: px, YHI: py // nyl, YLO: py % nyl}

    sent = []
    offsets = [(dx, dy) for dx in range(nx) for dy in range(ny) if (dx, dy) != (0, 0)]
    offsets.sort(key=lambda o: -(min(o[0], nx - o[0]) + min(o[1], ny - o[1])))

    barrier = pltpu.get_barrier_semaphore()

    def greet(where):
        pl.semaphore_signal(barrier, inc=1, device_id=where, device_id_type=MESH)

    for d in range(1, nzh):
        greet({Z: ((zh + d) % nzh) * nzl + zl})
    for d in range(1, nzl):
        greet({Z: zh * nzl + (zl + d) % nzl})
    for dx, dy in offsets:
        greet(at_plane(dx, dy)[1])
    greet({CORE: 1 - core})
    greet({CORE: 1 - core, YHI: 1 - yh})

    @pl.when(row < rows - 1)
    def _():
        greet(at_row(row + 1) | at_col(0))

    met = (nzh - 1) + (nzl - 1) + len(offsets) + 2

    load_g.wait()
    blocks = 4
    width = gsend.shape[1]
    sel_row, sel_col = iota((16, width), 0), iota((16, width), 1)
    for c in range(blocks - 1):
        hit = sel_col == 128 * (c + 1)
        first = jnp.where(hit & (sel_row == 0), 1.0, 0.0).astype(BF16)
        second = jnp.where(hit & (sel_row == 1), 1.0, 0.0).astype(BF16)
        tile = dot_nt(first, gsend[0:128, :]) + dot_nt(second, gsend[64:192, :])
        gsend[C : C + 16, 128 * c : 128 * c + 128] = tile.astype(BF16)
    gsend[C : C + 16, 128 * (blocks - 1) :] = jnp.zeros((16, 128), BF16)
    own = pl.multiple_of(col * 128, 128)
    gcat[:, pl.ds(own, 128)] = gsend[:, pl.ds(own, 128)]

    @pl.when(row == rows - 1)
    def _():
        gcat[:, 512:640] = jnp.zeros((C + 16, 128), BF16)

    @pl.when((col == 0) & (row > 0))
    def _():
        pl.semaphore_wait(barrier, met + 4)

    @pl.when((col != 0) | (row == 0))
    def _():
        pl.semaphore_wait(barrier, met)

    def g_copy(c, slot, where, sem):
        return pltpu.make_async_remote_copy(
            src_ref=gsend.at[:, pl.ds(pl.multiple_of(c * 128, 128), 128)],
            dst_ref=gcat.at[:, pl.ds(pl.multiple_of(slot * 128, 128), 128)],
            send_sem=gs_sem.at[sem], recv_sem=gr_sem.at[slot], device_id=where, device_id_type=MESH)

    peers = [(col + d) % 4 for d in (2, 3, 1)]
    for n, c in enumerate(peers):
        copy = g_copy(c, col, at_col(c), n)
        copy.start()
        sent.append(copy)
    upward = [g_copy(c, 4, at_row(row - 1) | at_col(c), 3 + c) for c in range(4)]

    @pl.when((col == 0) & (row > 0))
    def _():
        for copy in upward:
            copy.start()

    load_x.wait()
    r256, c256 = iota((256, 256), 0), iota((256, 256), 1)
    part = jnp.where(r256 == 2 * (c256 % 128) + c256 // 128, 1.0, 0.0).astype(BF16)
    join = jnp.where(c256 == 2 * (r256 % 128) + r256 // 128, 1.0, 0.0).astype(BF16)
    for p in range(8):
        both = dot_nn(xin[p], part).astype(BF16)
        lanes = slice(128 * (p // 2), 128 * (p // 2) + 128)
        xd[p % 2, 0, :, lanes] = both[:, 0:128]
        xd[p % 2, 1, :, lanes] = both[:, 128:256]

    for d in (1, 2, 3):
        g_copy(0, (col + d) % 4, at_col(0), 0).wait_recv()

    @pl.when(row < rows - 1)
    def _():
        g_copy(0, 4, at_col(0), 0).wait_recv()

    r128, c128 = iota((128, 128), 0), iota((128, 128), 1)
    shift = jnp.where(r128 == c128 + 1, 1.0, 0.0).astype(BF16)
    eye = jnp.where(r128 == c128, 1.0, 0.0).astype(BF16)
    for i in range(5):
        lanes = slice(128 * i, 128 * i + 128)
        moved = dot_nn(gcat[0:C, lanes], shift)
        tile = gcat[C : C + 16, lanes].astype(F32)
        edge0 = jnp.where(r128 == 127, tile[0:1, :], 0.0).astype(BF16)
        edge1 = jnp.where(r128 == 127, tile[1:2, :], 0.0).astype(BF16)
        gshift[0:128, lanes] = (moved[0:128] + dot_nt(eye, edge0)).astype(BF16)
        gshift[128:192, lanes] = (moved[128:192] + dot_nt(eye, edge1)[64:128]).astype(BF16)

    def grad(down, right):
        ref = gshift if right else gcat
        return ref, slice(128 * down, 128 * down + 512)

    taps = {0: (1, 1), 1: (0, 0), 2: (1, 0)}
    low = iota((C // 2, 128), 1) < 64
    for t in range(9):
        (row_par, down), (col_par, right) = taps[t // 3], taps[t % 3]
        ref, lanes = grad(down, right)
        lhs = xd[row_par, col_par]
        main = dot_nt(lhs, ref[0:128, lanes])
        rest = dot_nt(lhs, ref[64:192, lanes])
        rest = jnp.where(low, pltpu.roll(rest[0 : C // 2], 64, 1), rest[C // 2 : C])
        start = TAP_ROWS * t
        for begin, values in ((start, main), (start + C, rest)):
            count = values.shape[0]
            cut = min(max(HALF - begin, 0), count)
            if cut > 0:
                terms[0, begin : begin + cut] = values[0:cut]
            if cut < count:
                terms[1, begin + cut - HALF : begin + count - HALF] = values[cut:]
    spare = planes * chunk - HALF
    if spare:
        for h in range(2):
            terms[h, HALF:] = jnp.zeros((spare, 128), F32)

    pair = pltpu.make_async_remote_copy(
        src_ref=terms.at[1 - core], dst_ref=dbuf, send_sem=ds_sem, recv_sem=dr_sem,
        device_id={CORE: 1 - core}, device_id_type=MESH)
    pair.start()
    sent.append(pair)
    pair.wait_recv()

    def plane_copy(n, source, slot, where):
        return pltpu.make_async_remote_copy(
            src_ref=sbuf.at[source], dst_ref=rbuf.at[slot], send_sem=xs_sem.at[n], recv_sem=xr_sem.at[slot],
            device_id=where, device_id_type=MESH)

    for n, (dx, dy) in enumerate(offsets):
        q, where = at_plane(dx, dy)
        at = pl.ds(pl.multiple_of(q * chunk, chunk), chunk)
        sbuf[q] = (terms[core, at, :] + dbuf[at, :]).astype(BF16)
        copy = plane_copy(n, q, me, where)
        copy.start()
        sent.append(copy)
    at = pl.ds(pl.multiple_of(me * chunk, chunk), chunk)
    acc[...] = terms[core, at, :] + dbuf[at, :]

    load_w.wait()

    def tap(a, b):
        return w[3 * a + b]

    def apply(pairs):
        total = None
        for (a, b), (down, right) in pairs:
            ref, lanes = grad(down, right)
            one = dot_nn(tap(a, b), ref[0:C, lanes])
            total = one if total is None else total + one
        return total.astype(BF16)

    plan = {
        (0, 0): [((1, 1), (0, 0))],
        (0, 1): [((1, 2), (0, 0)), ((1, 0), (0, 1))],
        (1, 0): [((2, 1), (0, 0)), ((0, 1), (1, 0))],
        (1, 1): [((2, 2), (0, 0)), ((2, 0), (0, 1)), ((0, 2), (1, 0)), ((0, 0), (1, 1))],
    }
    for (row_par, col_par), pairs in plan.items():
        placed = apply(pairs)
        for i in range(4):
            ig2[row_par, i, :, 128 * col_par : 128 * col_par + 128] = placed[:, 128 * i : 128 * i + 128]
    for p in range(8):
        igo[p] = dot_nn(ig2[p % 2, p // 2], join).astype(BF16)

    total = acc[...]
    for dx, dy in reversed(offsets):
        q, where = at_plane(dx, dy)
        plane_copy(0, q, q, where).wait_recv()
        total += rbuf[q].astype(F32)
    acc[...] = total

    def near_copy(n, k, slot, where):
        return pltpu.make_async_remote_copy(
            src_ref=acc.at[pl.ds(pl.multiple_of(k * piece, 8), piece)], dst_ref=zbuf.at[slot],
            send_sem=ns_sem.at[n], recv_sem=nr_sem.at[slot], device_id={Z: where}, device_id_type=MESH)

    for d in range(1, nzl):
        k = (zl + d) % nzl
        copy = near_copy(d - 1, k, zl, zh * nzl + k)
        copy.start()
        sent.append(copy)
    total = acc[pl.ds(pl.multiple_of(zl * piece, 8), piece)]
    for d in range(1, nzl):
        k = (zl + d) % nzl
        near_copy(0, k, k, z).wait_recv()
        total += zbuf[k]
    zown[...] = total
    zfar[zh] = total

    def far_copy(n, slot, where):
        return pltpu.make_async_remote_copy(
            src_ref=zown, dst_ref=zfar.at[slot], send_sem=fs_sem.at[n], recv_sem=fr_sem.at[slot],
            device_id={Z: where}, device_id_type=MESH)

    for n, d in enumerate(sorted(range(1, nzh), key=lambda d: -min(d, nzh - d))):
        copy = far_copy(n, zh, ((zh + d) % nzh) * nzl + zl)
        copy.start()
        sent.append(copy)
    for d in range(1, nzh):
        far_copy(0, (zh + d) % nzh, z).wait_recv()
    total = zfar[0]
    for k in range(1, nzh):
        total += zfar[k]
    mine = pl.ds(pl.multiple_of(zl * piece, 8), piece)
    fin[mine] = total

    def gather_copy(n, k, where):
        part_of = pl.ds(pl.multiple_of(k * piece, 8), piece)
        return pltpu.make_async_remote_copy(
            src_ref=fin.at[part_of], dst_ref=fin.at[part_of], send_sem=as_sem.at[n], recv_sem=ar_sem.at[k],
            device_id={Z: where}, device_id_type=MESH)

    for d in range(1, nzl):
        copy = gather_copy(d - 1, zl, zh * nzl + (zl + d) % nzl)
        copy.start()
        sent.append(copy)
    for d in range(1, nzl):
        gather_copy(0, (zl + d) % nzl, z).wait_recv()

    def ag_at(h, q):
        return agbuf.at[h, pl.ds(pl.multiple_of(q * chunk, chunk), chunk)]

    def spread_copy(n, q, where):
        return pltpu.make_async_remote_copy(
            src_ref=ag_at(core, q), dst_ref=ag_at(core, q), send_sem=os_sem.at[n], recv_sem=or_sem.at[q],
            device_id=where, device_id_type=MESH)

    def pass_copy(q, half):
        return pltpu.make_async_remote_copy(
            src_ref=ag_at(half, q), dst_ref=ag_at(half, q), send_sem=ps_sem.at[q], recv_sem=pr_sem.at[q],
            device_id={CORE: 1 - core}, device_id_type=MESH)

    agbuf[core, pl.ds(pl.multiple_of(me * chunk, chunk), chunk)] = fin[...].astype(BF16)
    for n, (dx, dy) in enumerate(offsets):
        copy = spread_copy(n, me, at_plane(dx, dy)[1])
        copy.start()
        sent.append(copy)
    copy = pass_copy(me, core)
    copy.start()
    sent.append(copy)
    for dx, dy in reversed(offsets):
        q = at_plane(dx, dy)[0]
        spread_copy(0, q, {}).wait_recv()
        copy = pass_copy(q, core)
        copy.start()
        sent.append(copy)
    for q in range(planes):
        pass_copy(q, 1 - core).wait_recv()

    for copy in sent:
        copy.wait_send()

    @pl.when((col == 0) & (row > 0))
    def _():
        for copy in upward:
            copy.wait_send()


def finish(scale, igo, agbuf, ig_hbm, fg_hbm, fgo, sem):
    store_ig = pltpu.make_async_copy(igo, ig_hbm, sem.at[9])
    store_ig.start()

    def packed(begin, count):
        cut = min(max(HALF - begin, 0), count)
        parts = []
        if cut > 0:
            parts.append(agbuf[0, begin : begin + cut])
        if cut < count:
            parts.append(agbuf[1, begin + cut - HALF : begin + count - HALF])
        values = parts[0] if len(parts) == 1 else jnp.concatenate(parts, axis=0)
        return values.astype(F32) * scale

    stores = []
    for t in range(9):
        start = TAP_ROWS * t
        fgo[t, :, 0:128] = packed(start, C)
        rest = packed(start + C, C // 2)
        fgo[t, 0 : C // 2, 128:C] = rest[:, 0:64]
        fgo[t, C // 2 : C, 128:C] = pltpu.roll(rest, 64, 1)[:, 0:64]
        store = pltpu.make_async_copy(fgo.at[t], fg_hbm.at[t], sem.at[t])
        store.start()
        stores.append(store)
    for store in stores:
        store.wait()
    store_ig.wait()


def near_size(nz):
    return 4 if nz % 4 == 0 and nz > 4 else max(nz // 2, 1)


def per_device(scale, grad_out, inputs, weight):
    nyl, nx, nz, nyh = (lax.axis_size(a) for a in (YLO, X, Z, YHI))
    planes = nx * nyl * nyh
    nzl = near_size(nz)
    chunk = -(-HALF // planes)
    chunk = -(-chunk // 96) * 96
    g = jnp.transpose(grad_out, (0, 2, 1)).reshape(C, grad_out.shape[1])
    xt = jnp.transpose(inputs, (0, 2, 1))
    wt = weight.reshape(9, C, C)
    sizes = (nyl, nx, nz, nyh, nzl, chunk)
    dma = pltpu.SemaphoreType.DMA
    hbm = pl.BlockSpec(memory_space=pl.ANY)
    n = planes - 1
    nzh = nz // nzl
    piece = chunk // nzl
    vmem = pl.BlockSpec(memory_space=pltpu.VMEM)
    igo, agbuf = pl.pallas_call(
        functools.partial(kernel, sizes),
        out_shape=(pltpu.VMEM(xt.shape, BF16), pltpu.VMEM((2, planes * chunk, 128), BF16)),
        in_specs=[hbm] * 3,
        out_specs=(vmem, vmem),
        scratch_shapes=[
            pltpu.VMEM((C + 16, 512), BF16),
            pltpu.VMEM((C + 16, 640), BF16),
            pltpu.VMEM((C, 640), BF16),
            pltpu.VMEM(xt.shape, BF16),
            pltpu.VMEM((9, C, C), BF16),
            pltpu.VMEM((2, 2, C, 512), BF16),
            pltpu.VMEM((2, 4, C, 256), BF16),
            pltpu.VMEM((2, planes * chunk, 128), F32),
            pltpu.VMEM((planes * chunk, 128), F32),
            pltpu.VMEM((planes, chunk, 128), BF16),
            pltpu.VMEM((planes, chunk, 128), BF16),
            pltpu.VMEM((chunk, 128), F32),
            pltpu.VMEM((nzl, piece, 128), F32),
            pltpu.VMEM((nzh, piece, 128), F32),
            pltpu.VMEM((piece, 128), F32),
            pltpu.VMEM((chunk, 128), F32),
            dma((3,)), dma((7,)), dma((5,)), dma, dma, dma((n,)), dma((planes,)),
            dma((nzl,)), dma((nzl,)), dma((nzh,)), dma((nzh,)), dma((nzl,)), dma((nzl,)),
            dma((n,)), dma((planes,)), dma((planes,)), dma((planes,)),
        ],
        compiler_params=pltpu.CompilerParams(
            collective_id=0, has_side_effects=True, vmem_limit_bytes=65400000
        ),
    )(g, xt, wt)
    ig, fg = pl.pallas_call(
        functools.partial(finish, scale),
        out_shape=(jax.ShapeDtypeStruct(xt.shape, BF16), jax.ShapeDtypeStruct((9, C, C), F32)),
        in_specs=[vmem, vmem],
        out_specs=(hbm, hbm),
        scratch_shapes=[pltpu.VMEM((9, C, C), F32), dma((10,))],
        compiler_params=pltpu.CompilerParams(vmem_limit_bytes=16 * 1024 * 1024),
    )(igo, agbuf)
    return jnp.transpose(ig, (0, 2, 1)), fg.reshape(3, 3, C, C)


def solution(mesh):
    split = Mesh(mesh.devices.reshape(2, 4, 16, 2, 2), ROWS + COLS)
    positions = (4 * mesh.shape["rows"]) * (128 * mesh.shape["cols"])
    return jax.shard_map(
        functools.partial(per_device, positions ** -0.5),
        mesh=split,
        in_specs=(P(ROWS + COLS, None, None), P(ROWS, COLS, None), P()),
        out_specs=(P(ROWS, COLS, None), P()),
        check_vma=False,
    )
```
